32 devices in a mesh: ens: 2 (over y), gy: 4 (over z), gx: 4 (over x, core).
Axes of the slice: x: 2, y: 2, z: 4, core: 2. Of those that a mesh axis runs over, the one named last changes fastest.
Arguments:
- velocity: float32 [2, 2, 1024, 1024], P('ens', None, 'gy', 'gx'), may hold values from -3 to 3
- stress: float32 [2, 3, 1024, 1024], P('ens', None, 'gy', 'gx'), may hold values from -3 to 3
- thickness: float32 [2, 1024, 1024], P('ens', 'gy', 'gx'), may hold values from 2 to 3
- concentration: float32 [2, 1024, 1024], P('ens', 'gy', 'gx'), may hold values from 0.97 to 1
- node_mass: float32 [2, 1024, 1024], P('ens', 'gy', 'gx'), may hold values from 1 to 1.5
- wind_stress: float32 [2, 2, 1024, 1024], P('ens', None, 'gy', 'gx'), may hold values from -3 to 3
- ocean_current: float32 [2, 2, 1024, 1024], P('ens', None, 'gy', 'gx'), may hold values from -2 to 2
- ocean_mask: int32 [1024, 1024], P('gy', 'gx'), may hold values 0 or 1
- ice_blocks: int32 [2, 32, 32], P('ens', 'gy', 'gx'), may hold values 0 or 1
Outputs:
- velocity_out: float32 [2, 2, 1024, 1024], P('ens', None, 'gy', 'gx')
- stress_out: float32 [2, 3, 1024, 1024], P('ens', None, 'gy', 'gx')
- ensemble_mean: float32 [3, 1024, 1024], P(None, ('gy', 'ens'), 'gx')
- ensemble_variance: float32 [3, 1024, 1024], P(None, ('gy', 'ens'), 'gx')
The draws below stay inside these ranges and needn't reach their ends.
All inputs are finite; a program needn't handle non-finite values. No bound on the sum of `ocean_mask` or of `ice_blocks` on one device may be relied on, other than what follows from the above.
Results may differ from the reference program's by a relative error of at most 0.00002.
Values sent between devices are 32-bit elements; how exact they have to be, the bound alone decides.
A program may use at most 64 MiB of HBM per device.

```python
import math
import jax
import jax.numpy as jnp
from jax import lax

SUBCYCLES = 16
BLOCK = 32
MEMBERS = 2
NX = 1024
NY = 1024


def place_ends(entries, stream_key, low, high):
    extent = entries.shape
    place = [jax.random.randint(jax.random.fold_in(stream_key, axis), (), 0, extent[axis]) for axis in range(len(extent))]
    entries = entries.at[tuple(place)].set(low)
    longest = extent.index(max(extent))
    place[longest] = (place[longest] + 1) % extent[longest]
    return entries.at[tuple(place)].set(high)


def block_levels(key, dims, shards, smallest, largest):
    factor_of, own = 1.0, jax.random.fold_in(key, 6)
    for axis_at, shards_of in shards:
        draws = jnp.exp(jax.random.uniform(jax.random.fold_in(own, axis_at), (shards_of,), jnp.float32, smallest / len(shards), largest / len(shards)))
        factor_of = factor_of * jnp.repeat(draws, dims[axis_at] // shards_of).reshape([-1 if axis == axis_at else 1 for axis in range(len(dims))])
    return factor_of


def normal_values(rng, shape, scale, most, shards=(), kind=jnp.bfloat16):
    entries = jax.random.normal(rng, shape, jnp.float32) * scale
    if len(shards) > 0:
        entries = block_levels(rng, shape, shards, -0.22, 0.18) * entries
    return jnp.clip(entries, min=-most, max=most).astype(kind)


def setup_inputs(seed: int = 0) -> dict:
    key_list = jax.random.split(jax.random.key(seed), 10)
    return {
        "velocity": normal_values(key_list[0], (MEMBERS, 2, NY, NX), 0.5, 3.0, ((0, 2), (2, 4), (3, 4)), jnp.float32),
        "stress": normal_values(key_list[1], (MEMBERS, 3, NY, NX), 0.5, 3.0, ((0, 2), (2, 4), (3, 4)), jnp.float32),
        "thickness": jnp.clip(jnp.exp(math.log(3.0) - 0.4054651 * jax.random.uniform(key_list[2], (MEMBERS, NY, NX), jnp.float32) ** block_levels(key_list[2], (MEMBERS, NY, NX), ((0, 2), (1, 4), (2, 4)), -0.2, 0.2)), 2.0, 3.0),
        "concentration": jnp.clip(0.97 + 0.029999971 * jax.random.uniform(key_list[3], (MEMBERS, NY, NX), jnp.float32) ** block_levels(key_list[3], (MEMBERS, NY, NX), ((0, 2), (1, 4), (2, 4)), -0.2, 0.2), 0.97, 1.0),
        "node_mass": jnp.clip(jnp.exp(math.log(1.5) - 0.4054651 * jax.random.uniform(key_list[4], (MEMBERS, NY, NX), jnp.float32) ** block_levels(key_list[4], (MEMBERS, NY, NX), ((0, 2), (1, 4), (2, 4)), -0.2, 0.2)), 1.0, 1.5),
        "wind_stress": normal_values(key_list[5], (MEMBERS, 2, NY, NX), 0.5, 3.0, ((0, 2), (2, 4), (3, 4)), jnp.float32),
        "ocean_current": normal_values(key_list[6], (MEMBERS, 2, NY, NX), 0.3, 2.0, ((0, 2), (2, 4), (3, 4)), jnp.float32),
        "ocean_mask": place_ends((jax.random.randint(key_list[7], (NY, NX), 0, 5) < 4).astype(jnp.int32), jax.random.fold_in(key_list[7], 1), 0, 1),
        "ice_blocks": place_ends((jax.random.randint(key_list[8], (MEMBERS, NY // BLOCK, NX // BLOCK), 0, 4) < 3).astype(jnp.int32), jax.random.fold_in(key_list[8], 1), 0, 1),
    }


TIME_STEP = 0.5
RELAX_RATE = 0.25
ECCENTRICITY_SQUARED = 4.0
DELTA_FLOOR = 0.5
DRAG_WATER = 1.0
CORIOLIS_TOP = 1.0
STRENGTH_DECAY = 20.0
ADVECT_STEP = 1.0

def upper_extend(source):
    wrapped = jnp.concatenate([source, source[..., :1]], axis=-1)
    zeros_row = jnp.zeros_like(wrapped[..., :1, :])
    return jnp.concatenate([wrapped, zeros_row], axis=-2)

def lower_extend(source):
    wrapped = jnp.concatenate([source[..., -1:], source], axis=-1)
    zeros_row = jnp.zeros_like(wrapped[..., :1, :])
    return jnp.concatenate([zeros_row, wrapped], axis=-2)

def along_x(nodal_field):
    return 0.5 * (nodal_field[..., :-1, 1:] + nodal_field[..., 1:, 1:] - (nodal_field[..., :-1, :-1] + nodal_field[..., 1:, :-1]))

def along_y(nodal_field):
    return 0.5 * (nodal_field[..., 1:, :-1] + nodal_field[..., 1:, 1:] - (nodal_field[..., :-1, :-1] + nodal_field[..., :-1, 1:]))

def stress_update(stresses, extended_vel, strength):
    divergence = along_x(extended_vel[:, 0]) + along_y(extended_vel[:, 1])
    tension = along_x(extended_vel[:, 0]) - along_y(extended_vel[:, 1])
    shearing = along_y(extended_vel[:, 0]) + along_x(extended_vel[:, 1])
    deform = jnp.sqrt(divergence * divergence + (tension * tension + shearing * shearing) / ECCENTRICITY_SQUARED)
    bounded = jnp.maximum(deform, DELTA_FLOOR)
    weight = RELAX_RATE * 0.5 * strength / bounded
    stress_one = (stresses[:, 0] + weight * (divergence - deform)) / (1.0 + RELAX_RATE)
    stress_two = (stresses[:, 1] + weight * tension / ECCENTRICITY_SQUARED) / (1.0 + RELAX_RATE)
    stress_three = (stresses[:, 2] + weight * shearing / (2.0 * ECCENTRICITY_SQUARED)) / (1.0 + RELAX_RATE)
    return jnp.stack([stress_one, stress_two, stress_three], axis=1)

def momentum_update(moving, extended_stress, node_mass, wind_stress, ocean_current, coriolis, active):
    normal_east = 0.5 * (extended_stress[:, 0] + extended_stress[:, 1])
    normal_north = 0.5 * (extended_stress[:, 0] - extended_stress[:, 1])
    shear_part = extended_stress[:, 2]
    force_east = along_x(normal_east) + along_y(shear_part)
    force_north = along_x(shear_part) + along_y(normal_north)
    east_vel = moving[:, 0]
    north_vel = moving[:, 1]
    current_east = ocean_current[:, 0]
    current_north = ocean_current[:, 1]
    drag_rate = DRAG_WATER * jnp.sqrt((current_east - east_vel) * (current_east - east_vel) + (current_north - north_vel) * (current_north - north_vel))
    inertia = node_mass / TIME_STEP
    diagonal_term = inertia + drag_rate
    turning = coriolis * node_mass
    rhs_east = inertia * east_vel + force_east + wind_stress[:, 0] + drag_rate * current_east
    rhs_north = inertia * north_vel + force_north + wind_stress[:, 1] + drag_rate * current_north
    determinant = diagonal_term * diagonal_term + turning * turning
    new_east = active * (diagonal_term * rhs_east + turning * rhs_north) / determinant
    new_north = active * (diagonal_term * rhs_north - turning * rhs_east) / determinant
    return jnp.stack([new_east, new_north], axis=1)

def reference(velocity, stress, thickness, concentration, node_mass, wind_stress, ocean_current, ocean_mask, ice_blocks):
    present = jnp.repeat(jnp.repeat(ice_blocks, BLOCK, axis=1), BLOCK, axis=2).astype(jnp.float32)
    active = ocean_mask.astype(jnp.float32)[None] * present
    strength = thickness * jnp.exp(-STRENGTH_DECAY * (1.0 - concentration))
    row_index = jnp.arange(NY, dtype=jnp.int32).astype(jnp.float32)
    coriolis = (CORIOLIS_TOP * (row_index + 0.5) / NY)[:, None]
    initial = velocity * active[:, None]

    def subcycle(counter, carried):
        moving, stresses = carried
        stresses = stress_update(stresses, upper_extend(moving), strength)
        moving = momentum_update(moving, lower_extend(stresses), node_mass, wind_stress, ocean_current, coriolis, active)
        return (moving, stresses)
    final_vel, final_stress = lax.fori_loop(0, SUBCYCLES, subcycle, (initial, stress))
    extended = upper_extend(final_vel)
    divergence = along_x(extended[:, 0]) + along_y(extended[:, 1])
    drifted = jnp.clip(concentration - ADVECT_STEP * concentration * divergence, 0.0, 1.0)
    fields = jnp.stack([drifted, final_vel[:, 0], final_vel[:, 1]], axis=1)
    average = lax.optimization_barrier(jnp.sum(fields, axis=0)) / MEMBERS
    deviation = fields - average[None]
    spread = lax.optimization_barrier(jnp.sum(deviation * deviation, axis=0)) / MEMBERS
    return (final_vel, final_stress, average, spread)
```

```python
import functools

import jax
import jax.numpy as jnp
from jax import lax
from jax.experimental import pallas as pl
from jax.experimental.pallas import tpu as pltpu
from jax.sharding import PartitionSpec as P

SUBCYCLES = 16
BLOCK = 32

TIME_STEP = 0.5
RELAX_RATE = 0.25
ECCENTRICITY_SQUARED = 4.0
DELTA_FLOOR = 0.5
CORIOLIS_TOP = 1.0
STRENGTH_DECAY = 20.0

MESH = pl.DeviceIdType.MESH
LANES = 128
MARGIN = SUBCYCLES
EXTRA = 8
WIDE = 18
FIELDS = 12
PER_TILE = LANES // WIDE
X_TILES = -(-FIELDS // PER_TILE)
PER_CORNER = LANES // (2 * WIDE)
C_TILES = -(-FIELDS // PER_CORNER)
TOP = 8
STEP = 32
TINY = 1.1754944e-38


def lane_index(rows):
    return lax.broadcasted_iota(jnp.int32, (rows, LANES), 1)


def rolled(value, shift):
    shift = shift % LANES
    return value if shift == 0 else pltpu.roll(value, shift, 1)


def exchange_kernel(
    sizes,
    vel, stress, thick, conc, mass, wind, cur, mask, ice,
    derived, halo, rows_lo, rows_hi,
    x_out, x_in, y_up, y_dn, in_hi, in_lo, c_up, c_dn, cin_hi, cin_lo,
    send_sem, recv_sem,
):
    gx_count, gy_count = sizes
    rows, cols = thick.shape
    gx, gy = lax.axis_index("gx"), lax.axis_index("gy")
    right, left = lax.rem(gx + 1, gx_count), lax.rem(gx + gx_count - 1, gx_count)
    has_lo, has_hi = gy > 0, gy < gy_count - 1
    lower, upper = jnp.maximum(gy - 1, 0), jnp.minimum(gy + 1, gy_count - 1)

    barrier = pltpu.get_barrier_semaphore()
    for side in (left, right):
        pl.semaphore_signal(barrier, inc=1, device_id={"gx": side}, device_id_type=MESH)

    @pl.when(has_lo)
    def _():
        pl.semaphore_signal(barrier, inc=1, device_id={"gy": lower}, device_id_type=MESH)

    @pl.when(has_hi)
    def _():
        pl.semaphore_signal(barrier, inc=1, device_id={"gy": upper}, device_id_type=MESH)

    block_rows, block_cols = ice.shape
    spread_rows = (
        lax.broadcasted_iota(jnp.int32, (rows, block_rows), 0) // BLOCK
        == lax.broadcasted_iota(jnp.int32, (rows, block_rows), 1)
    ).astype(jnp.float32)
    spread_cols = (
        lax.broadcasted_iota(jnp.int32, (block_cols, cols), 1) // BLOCK
        == lax.broadcasted_iota(jnp.int32, (block_cols, cols), 0)
    ).astype(jnp.float32)
    present = jnp.dot(
        jnp.dot(spread_rows, ice[...].astype(jnp.float32), preferred_element_type=jnp.float32),
        spread_cols,
        preferred_element_type=jnp.float32,
    )
    derived[0] = thick[...] * jnp.exp(-STRENGTH_DECAY * (1.0 - conc[...]))
    derived[1] = mask[...].astype(jnp.float32) * present

    def field(f, r, c):
        if f < 2:
            return vel[f, r, c] * derived[1, r, c]
        if f < 5:
            return stress[f - 2, r, c]
        if f == 5:
            return derived[0, r, c]
        if f == 6:
            return mass[r, c]
        if f < 9:
            return wind[f - 7, r, c]
        if f < 11:
            return cur[f - 9, r, c]
        return derived[1, r, c]

    every = slice(0, rows)
    lanes = lane_index(rows)
    first, last = slice(0, LANES), slice(cols - LANES, cols)
    for tile in range(X_TILES):
        east = jnp.zeros((rows, LANES), jnp.float32)
        west = jnp.zeros((rows, LANES), jnp.float32)
        for f in range(tile * PER_TILE, min(FIELDS, (tile + 1) * PER_TILE)):
            at = (f - tile * PER_TILE) * WIDE
            here = jnp.logical_and(lanes >= at, lanes < at + WIDE)
            east = jnp.where(here, rolled(field(f, every, last), at - (LANES - WIDE)), east)
            west = jnp.where(here, rolled(field(f, every, first), at), west)
        x_out[0, tile] = east
        x_out[1, tile] = west
    wide = slice(0, cols)
    for f in range(FIELDS):
        at = slice(f * MARGIN, (f + 1) * MARGIN)
        y_up[at] = field(f, slice(0, MARGIN), wide)
        y_dn[at] = field(f, slice(rows - MARGIN, rows), wide)
    for f in range(2):
        at = FIELDS * MARGIN + f * EXTRA
        y_up[at : at + EXTRA] = field(f, slice(MARGIN, MARGIN + EXTRA), wide)

    def copy(source, target, number, where):
        return pltpu.make_async_remote_copy(
            src_ref=source,
            dst_ref=target,
            send_sem=send_sem.at[number],
            recv_sem=recv_sem.at[number],
            device_id=where,
            device_id_type=MESH,
        )

    to_right = copy(x_out.at[0], x_in.at[0], 0, {"gx": right})
    to_left = copy(x_out.at[1], x_in.at[1], 1, {"gx": left})
    to_lower = copy(y_up, in_hi, 2, {"gy": lower})
    to_upper = copy(y_dn, in_lo, 3, {"gy": upper})
    corner_lower = copy(c_up, cin_hi, 4, {"gy": lower})
    corner_upper = copy(c_dn, cin_lo, 5, {"gy": upper})

    pl.semaphore_wait(barrier, 2 + has_lo.astype(jnp.int32) + has_hi.astype(jnp.int32))
    to_right.start()
    to_left.start()

    @pl.when(has_lo)
    def _():
        to_lower.start()

    @pl.when(has_hi)
    def _():
        to_upper.start()

    to_right.wait_recv()
    to_left.wait_recv()
    for f in range(FIELDS):
        tile, at = f // PER_TILE, (f % PER_TILE) * WIDE
        from_right = rolled(x_in[1, tile], -at)
        from_left = rolled(x_in[0, tile], LANES - WIDE - at)
        halo[f, MARGIN : MARGIN + rows] = jnp.where(
            lanes < WIDE, from_right, jnp.where(lanes >= LANES - WIDE, from_left, 0.0)
        )

    def packed(start, count, tile):
        index = lane_index(count)
        total = jnp.zeros((count, LANES), jnp.float32)
        for f in range(tile * PER_CORNER, min(FIELDS, (tile + 1) * PER_CORNER)):
            at = (f - tile * PER_CORNER) * 2 * WIDE
            here = jnp.logical_and(index >= at, index < at + 2 * WIDE)
            total = jnp.where(here, rolled(halo[f, start : start + count], WIDE + at), total)
        return total

    for tile in range(C_TILES):
        at = slice(tile * MARGIN, (tile + 1) * MARGIN)
        c_up[at] = packed(MARGIN, MARGIN, tile)
        c_dn[at] = packed(rows, MARGIN, tile)
    c_up[C_TILES * MARGIN :] = packed(2 * MARGIN, EXTRA, 0)

    @pl.when(has_lo)
    def _():
        corner_lower.start()

    @pl.when(has_hi)
    def _():
        corner_upper.start()

    def unpacked(source, start, count, f):
        index = lane_index(count)
        value = rolled(source[start : start + count], -(WIDE + (f % PER_CORNER) * 2 * WIDE))
        return jnp.where(jnp.logical_or(index < WIDE, index >= LANES - WIDE), value, 0.0)

    @pl.when(has_lo)
    def _():
        to_upper.wait_recv()
        rows_lo[...] = in_lo[...]
        corner_upper.wait_recv()
        for f in range(FIELDS):
            halo[f, 0:MARGIN] = unpacked(cin_lo, f // PER_CORNER * MARGIN, MARGIN, f)

    @pl.when(jnp.logical_not(has_lo))
    def _():
        rows_lo[...] = jnp.zeros_like(rows_lo)
        for f in range(FIELDS):
            halo[f, 0:MARGIN] = jnp.zeros((MARGIN, LANES), jnp.float32)

    high = MARGIN + rows

    @pl.when(has_hi)
    def _():
        to_lower.wait_recv()
        rows_hi[...] = in_hi[...]
        corner_lower.wait_recv()
        for f in range(FIELDS):
            halo[f, high : high + MARGIN] = unpacked(cin_hi, f // PER_CORNER * MARGIN, MARGIN, f)
        for f in range(2):
            halo[f, high + MARGIN :] = unpacked(cin_hi, C_TILES * MARGIN, EXTRA, f)

    @pl.when(jnp.logical_not(has_hi))
    def _():
        rows_hi[...] = jnp.zeros_like(rows_hi)
        for f in range(FIELDS):
            halo[f, high : high + MARGIN] = jnp.zeros((MARGIN, LANES), jnp.float32)
        for f in range(2):
            halo[f, high + MARGIN :] = jnp.zeros((EXTRA, LANES), jnp.float32)

    for f in range(2, FIELDS):
        halo[f, high + MARGIN :] = jnp.zeros((EXTRA, LANES), jnp.float32)

    to_right.wait_send()
    to_left.wait_send()

    @pl.when(has_lo)
    def _():
        to_lower.wait_send()
        corner_lower.wait_send()

    @pl.when(has_hi)
    def _():
        to_upper.wait_send()
        corner_upper.wait_send()


def subcycle_kernel(
    gy_count,
    vel, stress, derived, conc, mass, wind, cur, halo, rows_lo, rows_hi,
    vel_out, stress_out, newconc,
    east, north, plus, minus, twice, pressure, inertia, turning,
    wind_e, wind_n, cur_e, cur_n, active,
):
    rows, cols = conc.shape
    main = cols // LANES
    tiles = main + 1
    low, mid, high = TOP, TOP + MARGIN, TOP + MARGIN + rows
    total = high + MARGIN + EXTRA
    gy = lax.axis_index("gy")

    def raw(f, r, c):
        if f < 2:
            return vel[f, r, c]
        if f < 5:
            return stress[f - 2, r, c]
        if f == 5:
            return derived[0, r, c]
        if f == 6:
            return mass[r, c]
        if f < 9:
            return wind[f - 7, r, c]
        if f < 11:
            return cur[f - 9, r, c]
        return derived[1, r, c]

    def piece(f, part, tile):
        if tile == main:
            bounds = (0, MARGIN, MARGIN + rows, 2 * MARGIN + rows, 2 * MARGIN + rows + EXTRA)
            return halo[f, bounds[part] : bounds[part + 1], :]
        c = slice(tile * LANES, (tile + 1) * LANES)
        if part == 0:
            return rows_lo[f * MARGIN : (f + 1) * MARGIN, c]
        if part == 1:
            return raw(f, slice(0, rows), c)
        if part == 2:
            return rows_hi[f * MARGIN : (f + 1) * MARGIN, c]
        start = FIELDS * MARGIN + f * EXTRA
        return rows_hi[start : start + EXTRA, c]

    spans = ((low, MARGIN), (mid, rows), (high, MARGIN))
    for tile in range(tiles):
        for part, (start, count) in enumerate(spans):
            at = slice(start, start + count)
            alive = piece(11, part, tile)
            active[tile, at] = alive
            east[tile, at] = piece(0, part, tile) * alive
            north[tile, at] = piece(1, part, tile) * alive
            one, two = piece(2, part, tile), piece(3, part, tile)
            plus[tile, at] = one + two
            minus[tile, at] = one - two
            twice[tile, at] = 2.0 * piece(4, part, tile)
            pressure[tile, at] = (RELAX_RATE * 0.5 / (1.0 + RELAX_RATE)) * piece(5, part, tile)
            heavy = piece(6, part, tile)
            heavy = jnp.where(heavy == 0.0, 1.0, heavy)
            inertia[tile, at] = heavy / TIME_STEP
            row = lax.broadcasted_iota(jnp.int32, (count, LANES), 0) + (gy * rows + (start - mid))
            coriolis = CORIOLIS_TOP * (row.astype(jnp.float32) + 0.5) / (rows * gy_count)
            turning[tile, at] = coriolis * heavy
            wind_e[tile, at] = piece(7, part, tile)
            wind_n[tile, at] = piece(8, part, tile)
            cur_e[tile, at] = piece(9, part, tile)
            cur_n[tile, at] = piece(10, part, tile)
        for ref in (plus, minus, twice):
            ref[tile, 0:low] = jnp.zeros((low, LANES), jnp.float32)
        east[tile, total - EXTRA : total] = piece(0, 3, tile)
        north[tile, total - EXTRA : total] = piece(1, 3, tile)

    lanes = lane_index(STEP)
    at_end, at_start = lanes == LANES - 1, lanes == 0

    def ahead(values):
        turned = [rolled(v, -1) for v in values]
        return [jnp.where(at_end, turned[(t + 1) % tiles], turned[t]) for t in range(tiles)]

    def behind(values):
        turned = [rolled(v, 1) for v in values]
        return [jnp.where(at_start, turned[t - 1], turned[t]) for t in range(tiles)]

    def gradients(start):
        add, sub, add_s, sub_s = [], [], [], []
        for t in range(tiles):
            u0, u1 = east[t, pl.ds(start, STEP)], east[t, pl.ds(start + 1, STEP)]
            v0, v1 = north[t, pl.ds(start, STEP)], north[t, pl.ds(start + 1, STEP)]
            a, b, c, d = u0 + u1, u1 - u0, v0 + v1, v1 - v0
            add.append(a + d)
            sub.append(a - d)
            add_s.append(b + c)
            sub_s.append(b - c)
        return add, sub, add_s, sub_s

    def stress_rows(start, growth):
        add, sub, add_s, sub_s = gradients(start)
        add_next, sub_next, shear_next = ahead(add), ahead(sub), ahead(add_s)
        for t in range(tiles):
            div = add_next[t] - sub[t]
            tension = sub_next[t] - add[t]
            shear = shear_next[t] + sub_s[t]
            square = div * div + (1.0 / ECCENTRICITY_SQUARED) * (tension * tension + shear * shear)
            inverse = lax.rsqrt(jnp.maximum(square, TINY))
            ratio = jnp.minimum(square * inverse, 1.0)
            force = pressure[t, pl.ds(start, STEP)] * growth
            weight = force * jnp.minimum(inverse, 1.0)
            quarter = weight * (1.0 / ECCENTRICITY_SQUARED)
            change = weight * div - force * ratio
            other = quarter * tension
            at = pl.ds(start, STEP)
            plus[t, at] = plus[t, at] + (change + other)
            minus[t, at] = minus[t, at] + (change - other)
            twice[t, at] = twice[t, at] + quarter * shear

    def velocity_rows(start, scale):
        at, before = pl.ds(start, STEP), pl.ds(start - 1, STEP)
        e_near, e_far, n_near, n_far = [], [], [], []
        for t in range(tiles):
            p1, p0 = plus[t, at], plus[t, before]
            m1, m0 = minus[t, at], minus[t, before]
            s1, s0 = twice[t, at], twice[t, before]
            a, d, b, e = p0 + p1, s1 - s0, s0 + s1, m1 - m0
            e_near.append(a + d)
            e_far.append(a - d)
            n_near.append(b + e)
            n_far.append(b - e)
        e_far, n_far = behind(e_far), behind(n_far)
        for t in range(tiles):
            force_e = (e_near[t] - e_far[t]) * scale
            force_n = (n_near[t] - n_far[t]) * scale
            u, v = east[t, at], north[t, at]
            ce, cn = cur_e[t, at], cur_n[t, at]
            de, dn = ce - u, cn - v
            square = de * de + dn * dn
            drag = square * lax.rsqrt(jnp.maximum(square, TINY))
            heavy, turn = inertia[t, at], turning[t, at]
            diag = heavy + drag
            re = heavy * u + force_e + wind_e[t, at] + drag * ce
            rn = heavy * v + force_n + wind_n[t, at] + drag * cn
            inverse = lax.rsqrt(diag * diag + turn * turn)
            inverse = active[t, at] * (inverse * inverse)
            east[t, at] = (diag * re + turn * rn) * inverse
            north[t, at] = (diag * rn - turn * re) * inverse

    blocks = (high + MARGIN - low) // STEP
    gain = 1.0 + RELAX_RATE

    def subcycle(number, carried):
        growth, scale = carried

        stress_rows(low, growth)

        def both(block, _):
            start = pl.multiple_of(low + block * STEP, 8)
            stress_rows(start, growth)
            velocity_rows(start - STEP, scale)
            return 0

        lax.fori_loop(1, blocks, both, 0)
        velocity_rows(low + (blocks - 1) * STEP, scale)
        return growth * gain, scale * (1.0 / gain)

    lax.fori_loop(
        0, SUBCYCLES, subcycle, (jnp.float32(gain), jnp.float32(0.25 / gain))
    )

    shrink = 0.5 * gain**-SUBCYCLES
    own = slice(mid, high)
    for t in range(main):
        c = slice(t * LANES, (t + 1) * LANES)
        vel_out[0, :, c] = east[t, own]
        vel_out[1, :, c] = north[t, own]
        stress_out[0, :, c] = (plus[t, own] + minus[t, own]) * shrink
        stress_out[1, :, c] = (plus[t, own] - minus[t, own]) * shrink
        stress_out[2, :, c] = twice[t, own] * shrink
    for block in range(rows // STEP):
        add, sub, _, _ = gradients(mid + block * STEP)
        add_next = ahead(add)
        at = slice(block * STEP, (block + 1) * STEP)
        for t in range(main):
            c = slice(t * LANES, (t + 1) * LANES)
            value = conc[at, c]
            newconc[at, c] = jnp.clip(value - value * (0.5 * (add_next[t] - sub[t])), 0.0, 1.0)


def ensemble_kernel(count, vel, newconc, mean, spread, land_vel, land_conc, send_sem, recv_sem):
    me = lax.axis_index("ens")
    share = newconc.shape[0] // count
    barrier = pltpu.get_barrier_semaphore()
    peers = [lax.rem(me + step, count) for step in range(1, count)]
    for peer in peers:
        pl.semaphore_signal(barrier, inc=1, device_id={"ens": peer}, device_id_type=MESH)
    pl.semaphore_wait(barrier, count - 1)
    copies = []
    for step, peer in enumerate(peers):
        at = pl.ds(pl.multiple_of(peer * share, 8), share)
        for kind, (source, target) in enumerate(
            ((vel.at[:, at], land_vel.at[step]), (newconc.at[at], land_conc.at[step]))
        ):
            each = pltpu.make_async_remote_copy(
                src_ref=source,
                dst_ref=target,
                send_sem=send_sem.at[kind, step],
                recv_sem=recv_sem.at[kind, step],
                device_id={"ens": peer},
                device_id_type=MESH,
            )
            each.start()
            copies.append(each)
    for each in copies:
        each.wait_recv()
    at = pl.ds(pl.multiple_of(me * share, 8), share)
    for f in range(3):
        own = newconc[at] if f == 0 else vel[f - 1, at]
        values = [own]
        for step in range(count - 1):
            values.append(land_conc[step] if f == 0 else land_vel[step, f - 1])
        average = functools.reduce(jnp.add, values) / count
        mean[f] = average
        squares = [(value - average) * (value - average) for value in values]
        spread[f] = functools.reduce(jnp.add, squares) / count
    for each in copies:
        each.wait_send()


def solution(mesh):
    gx_count, gy_count, ens_count = mesh.shape["gx"], mesh.shape["gy"], mesh.shape["ens"]
    f32 = jnp.float32

    def vmem(*shape):
        return pltpu.VMEM(shape, f32)

    def specs(count):
        return [pl.BlockSpec(memory_space=pltpu.VMEM)] * count

    def body(velocity, stress, thickness, concentration, node_mass, wind, current, mask, ice):
        rows, cols = mask.shape
        vel, stress = velocity[0], stress[0]
        conc, mass, wind, current = concentration[0], node_mass[0], wind[0], current[0]
        up_rows, dn_rows = FIELDS * MARGIN + 2 * EXTRA, FIELDS * MARGIN
        cu_rows, cd_rows = C_TILES * MARGIN + EXTRA, C_TILES * MARGIN
        tall = rows + 2 * MARGIN + EXTRA
        shape = lambda *dims: jax.ShapeDtypeStruct(dims, f32)
        derived, halo, rows_lo, rows_hi = pl.pallas_call(
            functools.partial(exchange_kernel, (gx_count, gy_count)),
            name="halo_exchange",
            out_shape=(
                shape(2, rows, cols),
                shape(FIELDS, tall, LANES),
                shape(dn_rows, cols),
                shape(up_rows, cols),
            ),
            in_specs=specs(9),
            out_specs=tuple(specs(4)),
            scratch_shapes=[
                vmem(2, X_TILES, rows, LANES),
                vmem(2, X_TILES, rows, LANES),
                vmem(up_rows, cols),
                vmem(dn_rows, cols),
                vmem(up_rows, cols),
                vmem(dn_rows, cols),
                vmem(cu_rows, LANES),
                vmem(cd_rows, LANES),
                vmem(cu_rows, LANES),
                vmem(cd_rows, LANES),
                pltpu.SemaphoreType.DMA((6,)),
                pltpu.SemaphoreType.DMA((6,)),
            ],
            compiler_params=pltpu.CompilerParams(collective_id=0, has_side_effects=True),
        )(vel, stress, thickness[0], conc, mass, wind, current, mask, ice[0])
        tiles = cols // LANES + 1
        vel_out, stress_out, newconc = pl.pallas_call(
            functools.partial(subcycle_kernel, gy_count),
            name="subcycles",
            out_shape=(shape(2, rows, cols), shape(3, rows, cols), shape(rows, cols)),
            in_specs=specs(10),
            out_specs=tuple(specs(3)),
            scratch_shapes=[vmem(tiles, TOP + tall, LANES)] * 13,
        )(vel, stress, derived, conc, mass, wind, current, halo, rows_lo, rows_hi)
        share = rows // ens_count
        mean, spread = pl.pallas_call(
            functools.partial(ensemble_kernel, ens_count),
            name="ensemble",
            out_shape=(shape(3, share, cols), shape(3, share, cols)),
            in_specs=specs(2),
            out_specs=tuple(specs(2)),
            scratch_shapes=[
                vmem(ens_count - 1, 2, share, cols),
                vmem(ens_count - 1, share, cols),
                pltpu.SemaphoreType.DMA((2, ens_count - 1)),
                pltpu.SemaphoreType.DMA((2, ens_count - 1)),
            ],
            compiler_params=pltpu.CompilerParams(collective_id=1, has_side_effects=True),
        )(vel_out, newconc)
        return vel_out[None], stress_out[None], mean, spread

    grid = P("ens", "gy", "gx")
    pair = P("ens", None, "gy", "gx")
    split = P(None, ("gy", "ens"), "gx")
    return jax.shard_map(
        body,
        mesh=mesh,
        in_specs=(pair, pair, grid, grid, grid, pair, pair, P("gy", "gx"), grid),
        out_specs=(pair, pair, split, split),
        check_vma=False,
    )
```

```python
import functools

import jax
import jax.numpy as jnp
from jax import lax
from jax.experimental import pallas as pl
from jax.experimental.pallas import tpu as pltpu
from jax.sharding import PartitionSpec as P

SUBCYCLES = 16
BLOCK = 32

TIME_STEP = 0.5
RELAX_RATE = 0.25
ECCENTRICITY_SQUARED = 4.0
DELTA_FLOOR = 0.5
CORIOLIS_TOP = 1.0
STRENGTH_DECAY = 20.0

MESH = pl.DeviceIdType.MESH
LANES = 128
MARGIN = SUBCYCLES
EXTRA = 8
WIDE = 18
FIELDS = 12
PER_TILE = LANES // WIDE
X_TILES = -(-FIELDS // PER_TILE)
PER_CORNER = LANES // (2 * WIDE)
C_TILES = -(-FIELDS // PER_CORNER)
TOP = 8
STEP = 32
TINY = 1.1754944e-38


def lane_index(rows):
    return lax.broadcasted_iota(jnp.int32, (rows, LANES), 1)


def rolled(value, shift):
    shift = shift % LANES
    return value if shift == 0 else pltpu.roll(value, shift, 1)


def exchange_kernel(
    sizes,
    vel, stress, thick, conc, mass, wind, cur, mask, ice,
    derived, halo, rows_lo, rows_hi,
    x_out, x_in, y_up, y_dn, in_hi, in_lo, c_up, c_dn, cin_hi, cin_lo,
    send_sem, recv_sem,
):
    gx_count, gy_count = sizes
    rows, cols = thick.shape
    gx, gy = lax.axis_index("gx"), lax.axis_index("gy")
    right, left = lax.rem(gx + 1, gx_count), lax.rem(gx + gx_count - 1, gx_count)
    has_lo, has_hi = gy > 0, gy < gy_count - 1
    lower, upper = jnp.maximum(gy - 1, 0), jnp.minimum(gy + 1, gy_count - 1)

    barrier = pltpu.get_barrier_semaphore()
    for side in (left, right):
        pl.semaphore_signal(barrier, inc=1, device_id={"gx": side}, device_id_type=MESH)

    @pl.when(has_lo)
    def _():
        pl.semaphore_signal(barrier, inc=1, device_id={"gy": lower}, device_id_type=MESH)

    @pl.when(has_hi)
    def _():
        pl.semaphore_signal(barrier, inc=1, device_id={"gy": upper}, device_id_type=MESH)

    block_rows, block_cols = ice.shape
    spread_rows = (
        lax.broadcasted_iota(jnp.int32, (rows, block_rows), 0) // BLOCK
        == lax.broadcasted_iota(jnp.int32, (rows, block_rows), 1)
    ).astype(jnp.float32)
    spread_cols = (
        lax.broadcasted_iota(jnp.int32, (block_cols, cols), 1) // BLOCK
        == lax.broadcasted_iota(jnp.int32, (block_cols, cols), 0)
    ).astype(jnp.float32)
    present = jnp.dot(
        jnp.dot(spread_rows, ice[...].astype(jnp.float32), preferred_element_type=jnp.float32),
        spread_cols,
        preferred_element_type=jnp.float32,
    )
    derived[0] = thick[...] * jnp.exp(-STRENGTH_DECAY * (1.0 - conc[...]))
    derived[1] = mask[...].astype(jnp.float32) * present

    def field(f, r, c):
        if f < 2:
            return vel[f, r, c] * derived[1, r, c]
        if f < 5:
            return stress[f - 2, r, c]
        if f == 5:
            return derived[0, r, c]
        if f == 6:
            return mass[r, c]
        if f < 9:
            return wind[f - 7, r, c]
        if f < 11:
            return cur[f - 9, r, c]
        return derived[1, r, c]

    every = slice(0, rows)
    lanes = lane_index(rows)
    first, last = slice(0, LANES), slice(cols - LANES, cols)
    for tile in range(X_TILES):
        east = jnp.zeros((rows, LANES), jnp.float32)
        west = jnp.zeros((rows, LANES), jnp.float32)
        for f in range(tile * PER_TILE, min(FIELDS, (tile + 1) * PER_TILE)):
            at = (f - tile * PER_TILE) * WIDE
            here = jnp.logical_and(lanes >= at, lanes < at + WIDE)
            east = jnp.where(here, rolled(field(f, every, last), at - (LANES - WIDE)), east)
            west = jnp.where(here, rolled(field(f, every, first), at), west)
        x_out[0, tile] = east
        x_out[1, tile] = west
    wide = slice(0, cols)
    for f in range(FIELDS):
        at = slice(f * MARGIN, (f + 1) * MARGIN)
        y_up[at] = field(f, slice(0, MARGIN), wide)
        y_dn[at] = field(f, slice(rows - MARGIN, rows), wide)
    for f in range(2):
        at = FIELDS * MARGIN + f * EXTRA
        y_up[at : at + EXTRA] = field(f, slice(MARGIN, MARGIN + EXTRA), wide)

    def copy(source, target, number, where):
        return pltpu.make_async_remote_copy(
            src_ref=source,
            dst_ref=target,
            send_sem=send_sem.at[number],
            recv_sem=recv_sem.at[number],
            device_id=where,
            device_id_type=MESH,
        )

    to_right = copy(x_out.at[0], x_in.at[0], 0, {"gx": right})
    to_left = copy(x_out.at[1], x_in.at[1], 1, {"gx": left})
    to_lower = copy(y_up, in_hi, 2, {"gy": lower})
    to_upper = copy(y_dn, in_lo, 3, {"gy": upper})
    corner_lower = copy(c_up, cin_hi, 4, {"gy": lower})
    corner_upper = copy(c_dn, cin_lo, 5, {"gy": upper})

    pl.semaphore_wait(barrier, 2 + has_lo.astype(jnp.int32) + has_hi.astype(jnp.int32))
    to_right.start()
    to_left.start()

    @pl.when(has_lo)
    def _():
        to_lower.start()

    @pl.when(has_hi)
    def _():
        to_upper.start()

    to_right.wait_recv()
    to_left.wait_recv()
    for f in range(FIELDS):
        tile, at = f // PER_TILE, (f % PER_TILE) * WIDE
        from_right = rolled(x_in[1, tile], -at)
        from_left = rolled(x_in[0, tile], LANES - WIDE - at)
        halo[f, MARGIN : MARGIN + rows] = jnp.where(
            lanes < WIDE, from_right, jnp.where(lanes >= LANES - WIDE, from_left, 0.0)
        )

    def packed(start, count, tile):
        index = lane_index(count)
        total = jnp.zeros((count, LANES), jnp.float32)
        for f in range(tile * PER_CORNER, min(FIELDS, (tile + 1) * PER_CORNER)):
            at = (f - tile * PER_CORNER) * 2 * WIDE
            here = jnp.logical_and(index >= at, index < at + 2 * WIDE)
            total = jnp.where(here, rolled(halo[f, start : start + count], WIDE + at), total)
        return total

    for tile in range(C_TILES):
        at = slice(tile * MARGIN, (tile + 1) * MARGIN)
        c_up[at] = packed(MARGIN, MARGIN, tile)
        c_dn[at] = packed(rows, MARGIN, tile)
    c_up[C_TILES * MARGIN :] = packed(2 * MARGIN, EXTRA, 0)

    @pl.when(has_lo)
    def _():
        corner_lower.start()

    @pl.when(has_hi)
    def _():
        corner_upper.start()

    def unpacked(source, start, count, f):
        index = lane_index(count)
        value = rolled(source[start : start + count], -(WIDE + (f % PER_CORNER) * 2 * WIDE))
        return jnp.where(jnp.logical_or(index < WIDE, index >= LANES - WIDE), value, 0.0)

    @pl.when(has_lo)
    def _():
        to_upper.wait_recv()
        rows_lo[...] = in_lo[...]
        corner_upper.wait_recv()
        for f in range(FIELDS):
            halo[f, 0:MARGIN] = unpacked(cin_lo, f // PER_CORNER * MARGIN, MARGIN, f)

    @pl.when(jnp.logical_not(has_lo))
    def _():
        rows_lo[...] = jnp.zeros_like(rows_lo)
        for f in range(FIELDS):
            halo[f, 0:MARGIN] = jnp.zeros((MARGIN, LANES), jnp.float32)

    high = MARGIN + rows

    @pl.when(has_hi)
    def _():
        to_lower.wait_recv()
        rows_hi[...] = in_hi[...]
        corner_lower.wait_recv()
        for f in range(FIELDS):
            halo[f, high : high + MARGIN] = unpacked(cin_hi, f // PER_CORNER * MARGIN, MARGIN, f)
        for f in range(2):
            halo[f, high + MARGIN :] = unpacked(cin_hi, C_TILES * MARGIN, EXTRA, f)

    @pl.when(jnp.logical_not(has_hi))
    def _():
        rows_hi[...] = jnp.zeros_like(rows_hi)
        for f in range(FIELDS):
            halo[f, high : high + MARGIN] = jnp.zeros((MARGIN, LANES), jnp.float32)
        for f in range(2):
            halo[f, high + MARGIN :] = jnp.zeros((EXTRA, LANES), jnp.float32)

    for f in range(2, FIELDS):
        halo[f, high + MARGIN :] = jnp.zeros((EXTRA, LANES), jnp.float32)

    to_right.wait_send()
    to_left.wait_send()

    @pl.when(has_lo)
    def _():
        to_lower.wait_send()
        corner_lower.wait_send()

    @pl.when(has_hi)
    def _():
        to_upper.wait_send()
        corner_upper.wait_send()


def subcycle_kernel(
    gy_count,
    vel, stress, derived, conc, mass, wind, cur, halo, rows_lo, rows_hi,
    vel_out, stress_out, fields,
    east, north, plus, minus, twice, pressure, inertia, turning,
    wind_e, wind_n, cur_e, cur_n, active,
):
    rows, cols = conc.shape
    main = cols // LANES
    tiles = main + 1
    low, mid, high = TOP, TOP + MARGIN, TOP + MARGIN + rows
    total = high + MARGIN + EXTRA
    gy = lax.axis_index("gy")

    def raw(f, r, c):
        if f < 2:
            return vel[f, r, c]
        if f < 5:
            return stress[f - 2, r, c]
        if f == 5:
            return derived[0, r, c]
        if f == 6:
            return mass[r, c]
        if f < 9:
            return wind[f - 7, r, c]
        if f < 11:
            return cur[f - 9, r, c]
        return derived[1, r, c]

    def piece(f, part, tile):
        if tile == main:
            bounds = (0, MARGIN, MARGIN + rows, 2 * MARGIN + rows, 2 * MARGIN + rows + EXTRA)
            return halo[f, bounds[part] : bounds[part + 1], :]
        c = slice(tile * LANES, (tile + 1) * LANES)
        if part == 0:
            return rows_lo[f * MARGIN : (f + 1) * MARGIN, c]
        if part == 1:
            return raw(f, slice(0, rows), c)
        if part == 2:
            return rows_hi[f * MARGIN : (f + 1) * MARGIN, c]
        start = FIELDS * MARGIN + f * EXTRA
        return rows_hi[start : start + EXTRA, c]

    spans = ((low, MARGIN), (mid, rows), (high, MARGIN))
    for tile in range(tiles):
        for part, (start, count) in enumerate(spans):
            at = slice(start, start + count)
            alive = piece(11, part, tile)
            active[tile, at] = alive
            east[tile, at] = piece(0, part, tile) * alive
            north[tile, at] = piece(1, part, tile) * alive
            one, two = piece(2, part, tile), piece(3, part, tile)
            plus[tile, at] = one + two
            minus[tile, at] = one - two
            twice[tile, at] = 2.0 * piece(4, part, tile)
            pressure[tile, at] = (RELAX_RATE * 0.5 / (1.0 + RELAX_RATE)) * piece(5, part, tile)
            heavy = piece(6, part, tile)
            heavy = jnp.where(heavy == 0.0, 1.0, heavy)
            inertia[tile, at] = heavy / TIME_STEP
            row = lax.broadcasted_iota(jnp.int32, (count, LANES), 0) + (gy * rows + (start - mid))
            coriolis = CORIOLIS_TOP * (row.astype(jnp.float32) + 0.5) / (rows * gy_count)
            turning[tile, at] = coriolis * heavy
            wind_e[tile, at] = piece(7, part, tile)
            wind_n[tile, at] = piece(8, part, tile)
            cur_e[tile, at] = piece(9, part, tile)
            cur_n[tile, at] = piece(10, part, tile)
        for ref in (plus, minus, twice):
            ref[tile, 0:low] = jnp.zeros((low, LANES), jnp.float32)
        east[tile, total - EXTRA : total] = piece(0, 3, tile)
        north[tile, total - EXTRA : total] = piece(1, 3, tile)

    lanes = lane_index(STEP)
    at_end, at_start = lanes == LANES - 1, lanes == 0

    def ahead(values):
        turned = [rolled(v, -1) for v in values]
        return [jnp.where(at_end, turned[(t + 1) % tiles], turned[t]) for t in range(tiles)]

    def behind(values):
        turned = [rolled(v, 1) for v in values]
        return [jnp.where(at_start, turned[t - 1], turned[t]) for t in range(tiles)]

    def gradients(start):
        add, sub, add_s, sub_s = [], [], [], []
        for t in range(tiles):
            u0, u1 = east[t, pl.ds(start, STEP)], east[t, pl.ds(start + 1, STEP)]
            v0, v1 = north[t, pl.ds(start, STEP)], north[t, pl.ds(start + 1, STEP)]
            a, b, c, d = u0 + u1, u1 - u0, v0 + v1, v1 - v0
            add.append(a + d)
            sub.append(a - d)
            add_s.append(b + c)
            sub_s.append(b - c)
        return add, sub, add_s, sub_s

    def stress_rows(start, growth):
        add, sub, add_s, sub_s = gradients(start)
        add_next, sub_next, shear_next = ahead(add), ahead(sub), ahead(add_s)
        for t in range(tiles):
            div = add_next[t] - sub[t]
            tension = sub_next[t] - add[t]
            shear = shear_next[t] + sub_s[t]
            square = div * div + (1.0 / ECCENTRICITY_SQUARED) * (tension * tension + shear * shear)
            inverse = lax.rsqrt(jnp.maximum(square, TINY))
            ratio = jnp.minimum(square * inverse, 1.0)
            force = pressure[t, pl.ds(start, STEP)] * growth
            weight = force * jnp.minimum(inverse, 1.0)
            quarter = weight * (1.0 / ECCENTRICITY_SQUARED)
            change = weight * div - force * ratio
            other = quarter * tension
            at = pl.ds(start, STEP)
            plus[t, at] = plus[t, at] + (change + other)
            minus[t, at] = minus[t, at] + (change - other)
            twice[t, at] = twice[t, at] + quarter * shear

    def velocity_rows(start, scale):
        at, before = pl.ds(start, STEP), pl.ds(start - 1, STEP)
        e_near, e_far, n_near, n_far = [], [], [], []
        for t in range(tiles):
            p1, p0 = plus[t, at], plus[t, before]
            m1, m0 = minus[t, at], minus[t, before]
            s1, s0 = twice[t, at], twice[t, before]
            a, d, b, e = p0 + p1, s1 - s0, s0 + s1, m1 - m0
            e_near.append(a + d)
            e_far.append(a - d)
            n_near.append(b + e)
            n_far.append(b - e)
        e_far, n_far = behind(e_far), behind(n_far)
        for t in range(tiles):
            force_e = (e_near[t] - e_far[t]) * scale
            force_n = (n_near[t] - n_far[t]) * scale
            u, v = east[t, at], north[t, at]
            ce, cn = cur_e[t, at], cur_n[t, at]
            de, dn = ce - u, cn - v
            square = de * de + dn * dn
            drag = square * lax.rsqrt(jnp.maximum(square, TINY))
            heavy, turn = inertia[t, at], turning[t, at]
            diag = heavy + drag
            re = heavy * u + force_e + wind_e[t, at] + drag * ce
            rn = heavy * v + force_n + wind_n[t, at] + drag * cn
            inverse = lax.rsqrt(diag * diag + turn * turn)
            inverse = active[t, at] * (inverse * inverse)
            east[t, at] = (diag * re + turn * rn) * inverse
            north[t, at] = (diag * rn - turn * re) * inverse

    blocks = (high + MARGIN - low) // STEP
    gain = 1.0 + RELAX_RATE

    def subcycle(number, carried):
        growth, scale = carried

        stress_rows(low, growth)

        def both(block, _):
            start = pl.multiple_of(low + block * STEP, 8)
            stress_rows(start, growth)
            velocity_rows(start - STEP, scale)
            return 0

        lax.fori_loop(1, blocks, both, 0)
        velocity_rows(low + (blocks - 1) * STEP, scale)
        return growth * gain, scale * (1.0 / gain)

    lax.fori_loop(
        0, SUBCYCLES, subcycle, (jnp.float32(gain), jnp.float32(0.25 / gain))
    )

    shrink = 0.5 * gain**-SUBCYCLES
    own = slice(mid, high)
    for t in range(main):
        c = slice(t * LANES, (t + 1) * LANES)
        vel_out[0, :, c] = fields[1, :, c] = east[t, own]
        vel_out[1, :, c] = fields[2, :, c] = north[t, own]
        stress_out[0, :, c] = (plus[t, own] + minus[t, own]) * shrink
        stress_out[1, :, c] = (plus[t, own] - minus[t, own]) * shrink
        stress_out[2, :, c] = twice[t, own] * shrink
    for block in range(rows // STEP):
        add, sub, _, _ = gradients(mid + block * STEP)
        add_next = ahead(add)
        at = slice(block * STEP, (block + 1) * STEP)
        for t in range(main):
            c = slice(t * LANES, (t + 1) * LANES)
            value = conc[at, c]
            fields[0, at, c] = jnp.clip(value - value * (0.5 * (add_next[t] - sub[t])), 0.0, 1.0)


def ensemble_kernel(count, fields, mean, spread, landing, send_sem, recv_sem):
    me = lax.axis_index("ens")
    share = mean.shape[1]
    barrier = pltpu.get_barrier_semaphore()
    peers = [lax.rem(me + step, count) for step in range(1, count)]
    for peer in peers:
        pl.semaphore_signal(barrier, inc=1, device_id={"ens": peer}, device_id_type=MESH)
    pl.semaphore_wait(barrier, count - 1)
    copies = []
    for step, peer in enumerate(peers):
        each = pltpu.make_async_remote_copy(
            src_ref=fields.at[:, pl.ds(pl.multiple_of(peer * share, 8), share)],
            dst_ref=landing.at[step],
            send_sem=send_sem.at[step],
            recv_sem=recv_sem.at[step],
            device_id={"ens": peer},
            device_id_type=MESH,
        )
        each.start()
        copies.append(each)
    for each in copies:
        each.wait_recv()
    own = fields[:, pl.ds(pl.multiple_of(me * share, 8), share)]
    values = [own] + [landing[step] for step in range(count - 1)]
    average = functools.reduce(jnp.add, values) / count
    mean[...] = average
    spread[...] = functools.reduce(jnp.add, [(v - average) * (v - average) for v in values]) / count
    for each in copies:
        each.wait_send()


def solution(mesh):
    gx_count, gy_count, ens_count = mesh.shape["gx"], mesh.shape["gy"], mesh.shape["ens"]
    f32 = jnp.float32

    def vmem(*shape):
        return pltpu.VMEM(shape, f32)

    def specs(count):
        return [pl.BlockSpec(memory_space=pltpu.VMEM)] * count

    def body(velocity, stress, thickness, concentration, node_mass, wind, current, mask, ice):
        rows, cols = mask.shape
        vel, stress = velocity[0], stress[0]
        conc, mass, wind, current = concentration[0], node_mass[0], wind[0], current[0]
        up_rows, dn_rows = FIELDS * MARGIN + 2 * EXTRA, FIELDS * MARGIN
        cu_rows, cd_rows = C_TILES * MARGIN + EXTRA, C_TILES * MARGIN
        tall = rows + 2 * MARGIN + EXTRA
        shape = lambda *dims: jax.ShapeDtypeStruct(dims, f32)
        derived, halo, rows_lo, rows_hi = pl.pallas_call(
            functools.partial(exchange_kernel, (gx_count, gy_count)),
            name="halo_exchange",
            out_shape=(
                shape(2, rows, cols),
                shape(FIELDS, tall, LANES),
                shape(dn_rows, cols),
                shape(up_rows, cols),
            ),
            in_specs=specs(9),
            out_specs=tuple(specs(4)),
            scratch_shapes=[
                vmem(2, X_TILES, rows, LANES),
                vmem(2, X_TILES, rows, LANES),
                vmem(up_rows, cols),
                vmem(dn_rows, cols),
                vmem(up_rows, cols),
                vmem(dn_rows, cols),
                vmem(cu_rows, LANES),
                vmem(cd_rows, LANES),
                vmem(cu_rows, LANES),
                vmem(cd_rows, LANES),
                pltpu.SemaphoreType.DMA((6,)),
                pltpu.SemaphoreType.DMA((6,)),
            ],
            compiler_params=pltpu.CompilerParams(collective_id=0, has_side_effects=True, vmem_limit_bytes=16 << 20),
        )(vel, stress, thickness[0], conc, mass, wind, current, mask, ice[0])
        tiles = cols // LANES + 1
        vel_out, stress_out, fields = pl.pallas_call(
            functools.partial(subcycle_kernel, gy_count),
            name="subcycles",
            out_shape=(shape(2, rows, cols), shape(3, rows, cols), shape(3, rows, cols)),
            in_specs=specs(10),
            out_specs=tuple(specs(3)),
            scratch_shapes=[vmem(tiles, TOP + tall, LANES)] * 13,
            compiler_params=pltpu.CompilerParams(vmem_limit_bytes=20 << 20),
        )(vel, stress, derived, conc, mass, wind, current, halo, rows_lo, rows_hi)
        share = rows // ens_count
        mean, spread = pl.pallas_call(
            functools.partial(ensemble_kernel, ens_count),
            name="ensemble",
            out_shape=(shape(3, share, cols), shape(3, share, cols)),
            in_specs=specs(1),
            out_specs=tuple(specs(2)),
            scratch_shapes=[
                vmem(ens_count - 1, 3, share, cols),
                pltpu.SemaphoreType.DMA((ens_count - 1,)),
                pltpu.SemaphoreType.DMA((ens_count - 1,)),
            ],
            compiler_params=pltpu.CompilerParams(collective_id=1, has_side_effects=True, vmem_limit_bytes=6 << 20),
        )(fields)
        return vel_out[None], stress_out[None], mean, spread

    grid = P("ens", "gy", "gx")
    pair = P("ens", None, "gy", "gx")
    split = P(None, ("gy", "ens"), "gx")
    return jax.shard_map(
        body,
        mesh=mesh,
        in_specs=(pair, pair, grid, grid, grid, pair, pair, P("gy", "gx"), grid),
        out_specs=(pair, pair, split, split),
        check_vma=False,
    )
```

```python
import functools

import jax
import jax.numpy as jnp
from jax import lax
from jax.experimental import pallas as pl
from jax.experimental.pallas import tpu as pltpu
from jax.sharding import PartitionSpec as P

SUBCYCLES = 16
BLOCK = 32

TIME_STEP = 0.5
RELAX_RATE = 0.25
ECCENTRICITY_SQUARED = 4.0
DELTA_FLOOR = 0.5
CORIOLIS_TOP = 1.0
STRENGTH_DECAY = 20.0

MESH = pl.DeviceIdType.MESH
LANES = 128
MARGIN = SUBCYCLES
EXTRA = 8
WIDE = 18
FIELDS = 12
PER_TILE = LANES // WIDE
X_TILES = -(-FIELDS // PER_TILE)
PER_CORNER = LANES // (2 * WIDE)
C_TILES = -(-FIELDS // PER_CORNER)
TOP = 8
STEP = 32
TINY = 1.1754944e-38


def lane_index(rows):
    return lax.broadcasted_iota(jnp.int32, (rows, LANES), 1)


def rolled(value, shift):
    shift = shift % LANES
    return value if shift == 0 else pltpu.roll(value, shift, 1)


def exchange_kernel(
    sizes,
    vel, stress, thick, conc, mass, wind, cur, mask, ice,
    derived, halo, rows_lo, rows_hi,
    x_out, x_in, y_up, y_dn, in_hi, in_lo, c_up, c_dn, cin_hi, cin_lo,
    send_sem, recv_sem,
):
    gx_count, gy_count = sizes
    rows, cols = thick.shape
    gx, gy = lax.axis_index("gx"), lax.axis_index("gy")
    right, left = lax.rem(gx + 1, gx_count), lax.rem(gx + gx_count - 1, gx_count)
    has_lo, has_hi = gy > 0, gy < gy_count - 1
    lower, upper = jnp.maximum(gy - 1, 0), jnp.minimum(gy + 1, gy_count - 1)

    barrier = pltpu.get_barrier_semaphore()
    for side in (left, right):
        pl.semaphore_signal(barrier, inc=1, device_id={"gx": side}, device_id_type=MESH)

    @pl.when(has_lo)
    def _():
        pl.semaphore_signal(barrier, inc=1, device_id={"gy": lower}, device_id_type=MESH)

    @pl.when(has_hi)
    def _():
        pl.semaphore_signal(barrier, inc=1, device_id={"gy": upper}, device_id_type=MESH)

    block_rows, block_cols = ice.shape
    spread_rows = (
        lax.broadcasted_iota(jnp.int32, (rows, block_rows), 0) // BLOCK
        == lax.broadcasted_iota(jnp.int32, (rows, block_rows), 1)
    ).astype(jnp.float32)
    spread_cols = (
        lax.broadcasted_iota(jnp.int32, (block_cols, cols), 1) // BLOCK
        == lax.broadcasted_iota(jnp.int32, (block_cols, cols), 0)
    ).astype(jnp.float32)
    present = jnp.dot(
        jnp.dot(spread_rows, ice[...].astype(jnp.float32), preferred_element_type=jnp.float32),
        spread_cols,
        preferred_element_type=jnp.float32,
    )
    derived[0] = thick[...] * jnp.exp(-STRENGTH_DECAY * (1.0 - conc[...]))
    derived[1] = mask[...].astype(jnp.float32) * present

    def field(f, r, c):
        if f < 2:
            return vel[f, r, c] * derived[1, r, c]
        if f < 5:
            return stress[f - 2, r, c]
        if f == 5:
            return derived[0, r, c]
        if f == 6:
            return mass[r, c]
        if f < 9:
            return wind[f - 7, r, c]
        if f < 11:
            return cur[f - 9, r, c]
        return derived[1, r, c]

    every = slice(0, rows)
    lanes = lane_index(rows)
    first, last = slice(0, LANES), slice(cols - LANES, cols)
    for tile in range(X_TILES):
        east = jnp.zeros((rows, LANES), jnp.float32)
        west = jnp.zeros((rows, LANES), jnp.float32)
        for f in range(tile * PER_TILE, min(FIELDS, (tile + 1) * PER_TILE)):
            at = (f - tile * PER_TILE) * WIDE
            here = jnp.logical_and(lanes >= at, lanes < at + WIDE)
            east = jnp.where(here, rolled(field(f, every, last), at - (LANES - WIDE)), east)
            west = jnp.where(here, rolled(field(f, every, first), at), west)
        x_out[0, tile] = east
        x_out[1, tile] = west
    def copy(source, target, number, where):
        return pltpu.make_async_remote_copy(
            src_ref=source,
            dst_ref=target,
            send_sem=send_sem.at[number],
            recv_sem=recv_sem.at[number],
            device_id=where,
            device_id_type=MESH,
        )

    to_right = copy(x_out.at[0], x_in.at[0], 0, {"gx": right})
    to_left = copy(x_out.at[1], x_in.at[1], 1, {"gx": left})
    to_lower = copy(y_up, in_hi, 2, {"gy": lower})
    to_upper = copy(y_dn, in_lo, 3, {"gy": upper})
    corner_lower = copy(c_up, cin_hi, 4, {"gy": lower})
    corner_upper = copy(c_dn, cin_lo, 5, {"gy": upper})

    pl.semaphore_wait(barrier, 2 + has_lo.astype(jnp.int32) + has_hi.astype(jnp.int32))
    to_right.start()
    to_left.start()

    wide = slice(0, cols)
    for f in range(FIELDS):
        at = slice(f * MARGIN, (f + 1) * MARGIN)
        y_up[at] = field(f, slice(0, MARGIN), wide)
        y_dn[at] = field(f, slice(rows - MARGIN, rows), wide)
    for f in range(2):
        at = FIELDS * MARGIN + f * EXTRA
        y_up[at : at + EXTRA] = field(f, slice(MARGIN, MARGIN + EXTRA), wide)

    @pl.when(has_lo)
    def _():
        to_lower.start()

    @pl.when(has_hi)
    def _():
        to_upper.start()

    to_right.wait_recv()
    to_left.wait_recv()
    for f in range(FIELDS):
        tile, at = f // PER_TILE, (f % PER_TILE) * WIDE
        from_right = rolled(x_in[1, tile], -at)
        from_left = rolled(x_in[0, tile], LANES - WIDE - at)
        halo[f, MARGIN : MARGIN + rows] = jnp.where(
            lanes < WIDE, from_right, jnp.where(lanes >= LANES - WIDE, from_left, 0.0)
        )

    def packed(start, count, tile):
        index = lane_index(count)
        total = jnp.zeros((count, LANES), jnp.float32)
        for f in range(tile * PER_CORNER, min(FIELDS, (tile + 1) * PER_CORNER)):
            at = (f - tile * PER_CORNER) * 2 * WIDE
            here = jnp.logical_and(index >= at, index < at + 2 * WIDE)
            total = jnp.where(here, rolled(halo[f, start : start + count], WIDE + at), total)
        return total

    for tile in range(C_TILES):
        at = slice(tile * MARGIN, (tile + 1) * MARGIN)
        c_up[at] = packed(MARGIN, MARGIN, tile)
        c_dn[at] = packed(rows, MARGIN, tile)
    c_up[C_TILES * MARGIN :] = packed(2 * MARGIN, EXTRA, 0)

    @pl.when(has_lo)
    def _():
        corner_lower.start()

    @pl.when(has_hi)
    def _():
        corner_upper.start()

    def unpacked(source, start, count, f):
        index = lane_index(count)
        value = rolled(source[start : start + count], -(WIDE + (f % PER_CORNER) * 2 * WIDE))
        return jnp.where(jnp.logical_or(index < WIDE, index >= LANES - WIDE), value, 0.0)

    @pl.when(has_lo)
    def _():
        to_upper.wait_recv()
        rows_lo[...] = in_lo[...]
        corner_upper.wait_recv()
        for f in range(FIELDS):
            halo[f, 0:MARGIN] = unpacked(cin_lo, f // PER_CORNER * MARGIN, MARGIN, f)

    @pl.when(jnp.logical_not(has_lo))
    def _():
        rows_lo[...] = jnp.zeros_like(rows_lo)
        for f in range(FIELDS):
            halo[f, 0:MARGIN] = jnp.zeros((MARGIN, LANES), jnp.float32)

    high = MARGIN + rows

    @pl.when(has_hi)
    def _():
        to_lower.wait_recv()
        rows_hi[...] = in_hi[...]
        corner_lower.wait_recv()
        for f in range(FIELDS):
            halo[f, high : high + MARGIN] = unpacked(cin_hi, f // PER_CORNER * MARGIN, MARGIN, f)
        for f in range(2):
            halo[f, high + MARGIN :] = unpacked(cin_hi, C_TILES * MARGIN, EXTRA, f)

    @pl.when(jnp.logical_not(has_hi))
    def _():
        rows_hi[...] = jnp.zeros_like(rows_hi)
        for f in range(FIELDS):
            halo[f, high : high + MARGIN] = jnp.zeros((MARGIN, LANES), jnp.float32)
        for f in range(2):
            halo[f, high + MARGIN :] = jnp.zeros((EXTRA, LANES), jnp.float32)

    for f in range(2, FIELDS):
        halo[f, high + MARGIN :] = jnp.zeros((EXTRA, LANES), jnp.float32)

    to_right.wait_send()
    to_left.wait_send()

    @pl.when(has_lo)
    def _():
        to_lower.wait_send()
        corner_lower.wait_send()

    @pl.when(has_hi)
    def _():
        to_upper.wait_send()
        corner_upper.wait_send()


def subcycle_kernel(
    gy_count,
    vel, stress, derived, conc, mass, wind, cur, halo, rows_lo, rows_hi,
    vel_out, stress_out, fields,
    east, north, plus, minus, twice, pressure, inertia, turning,
    wind_e, wind_n, cur_e, cur_n, active,
):
    rows, cols = conc.shape
    main = cols // LANES
    tiles = main + 1
    low, mid, high = TOP, TOP + MARGIN, TOP + MARGIN + rows
    total = high + MARGIN + EXTRA
    gy = lax.axis_index("gy")

    def raw(f, r, c):
        if f < 2:
            return vel[f, r, c]
        if f < 5:
            return stress[f - 2, r, c]
        if f == 5:
            return derived[0, r, c]
        if f == 6:
            return mass[r, c]
        if f < 9:
            return wind[f - 7, r, c]
        if f < 11:
            return cur[f - 9, r, c]
        return derived[1, r, c]

    def piece(f, part, tile):
        if tile == main:
            bounds = (0, MARGIN, MARGIN + rows, 2 * MARGIN + rows, 2 * MARGIN + rows + EXTRA)
            return halo[f, bounds[part] : bounds[part + 1], :]
        c = slice(tile * LANES, (tile + 1) * LANES)
        if part == 0:
            return rows_lo[f * MARGIN : (f + 1) * MARGIN, c]
        if part == 1:
            return raw(f, slice(0, rows), c)
        if part == 2:
            return rows_hi[f * MARGIN : (f + 1) * MARGIN, c]
        start = FIELDS * MARGIN + f * EXTRA
        return rows_hi[start : start + EXTRA, c]

    spans = ((low, MARGIN), (mid, rows), (high, MARGIN))
    for tile in range(tiles):
        for part, (start, count) in enumerate(spans):
            at = slice(start, start + count)
            alive = piece(11, part, tile)
            active[tile, at] = alive
            east[tile, at] = piece(0, part, tile) * alive
            north[tile, at] = piece(1, part, tile) * alive
            one, two = piece(2, part, tile), piece(3, part, tile)
            plus[tile, at] = one + two
            minus[tile, at] = one - two
            twice[tile, at] = 2.0 * piece(4, part, tile)
            pressure[tile, at] = (RELAX_RATE * 0.5 / (1.0 + RELAX_RATE)) * piece(5, part, tile)
            heavy = piece(6, part, tile)
            heavy = jnp.where(heavy == 0.0, 1.0, heavy)
            inertia[tile, at] = heavy / TIME_STEP
            row = lax.broadcasted_iota(jnp.int32, (count, LANES), 0) + (gy * rows + (start - mid))
            coriolis = CORIOLIS_TOP * (row.astype(jnp.float32) + 0.5) / (rows * gy_count)
            turning[tile, at] = coriolis * heavy
            wind_e[tile, at] = piece(7, part, tile)
            wind_n[tile, at] = piece(8, part, tile)
            cur_e[tile, at] = piece(9, part, tile)
            cur_n[tile, at] = piece(10, part, tile)
        for ref in (plus, minus, twice):
            ref[tile, 0:low] = jnp.zeros((low, LANES), jnp.float32)
        east[tile, total - EXTRA : total] = piece(0, 3, tile)
        north[tile, total - EXTRA : total] = piece(1, 3, tile)

    lanes = lane_index(STEP)
    at_end, at_start = lanes == LANES - 1, lanes == 0

    def ahead(values):
        turned = [rolled(v, -1) for v in values]
        return [jnp.where(at_end, turned[(t + 1) % tiles], turned[t]) for t in range(tiles)]

    def behind(values):
        turned = [rolled(v, 1) for v in values]
        return [jnp.where(at_start, turned[t - 1], turned[t]) for t in range(tiles)]

    def gradients(start):
        add, sub, add_s, sub_s = [], [], [], []
        for t in range(tiles):
            u0, u1 = east[t, pl.ds(start, STEP)], east[t, pl.ds(start + 1, STEP)]
            v0, v1 = north[t, pl.ds(start, STEP)], north[t, pl.ds(start + 1, STEP)]
            a, b, c, d = u0 + u1, u1 - u0, v0 + v1, v1 - v0
            add.append(a + d)
            sub.append(a - d)
            add_s.append(b + c)
            sub_s.append(b - c)
        return add, sub, add_s, sub_s

    def stress_rows(start, growth):
        add, sub, add_s, sub_s = gradients(start)
        add_next, sub_next, shear_next = ahead(add), ahead(sub), ahead(add_s)
        for t in range(tiles):
            div = add_next[t] - sub[t]
            tension = sub_next[t] - add[t]
            shear = shear_next[t] + sub_s[t]
            square = div * div + (1.0 / ECCENTRICITY_SQUARED) * (tension * tension + shear * shear)
            inverse = lax.rsqrt(jnp.maximum(square, TINY))
            ratio = jnp.minimum(square * inverse, 1.0)
            force = pressure[t, pl.ds(start, STEP)] * growth
            weight = force * jnp.minimum(inverse, 1.0)
            quarter = weight * (1.0 / ECCENTRICITY_SQUARED)
            change = weight * div - force * ratio
            other = quarter * tension
            at = pl.ds(start, STEP)
            plus[t, at] = plus[t, at] + (change + other)
            minus[t, at] = minus[t, at] + (change - other)
            twice[t, at] = twice[t, at] + quarter * shear

    def velocity_rows(start, scale):
        at, before = pl.ds(start, STEP), pl.ds(start - 1, STEP)
        e_near, e_far, n_near, n_far = [], [], [], []
        for t in range(tiles):
            p1, p0 = plus[t, at], plus[t, before]
            m1, m0 = minus[t, at], minus[t, before]
            s1, s0 = twice[t, at], twice[t, before]
            a, d, b, e = p0 + p1, s1 - s0, s0 + s1, m1 - m0
            e_near.append(a + d)
            e_far.append(a - d)
            n_near.append(b + e)
            n_far.append(b - e)
        e_far, n_far = behind(e_far), behind(n_far)
        for t in range(tiles):
            force_e = (e_near[t] - e_far[t]) * scale
            force_n = (n_near[t] - n_far[t]) * scale
            u, v = east[t, at], north[t, at]
            ce, cn = cur_e[t, at], cur_n[t, at]
            de, dn = ce - u, cn - v
            square = de * de + dn * dn
            drag = square * lax.rsqrt(jnp.maximum(square, TINY))
            heavy, turn = inertia[t, at], turning[t, at]
            diag = heavy + drag
            re = heavy * u + force_e + wind_e[t, at] + drag * ce
            rn = heavy * v + force_n + wind_n[t, at] + drag * cn
            inverse = lax.rsqrt(diag * diag + turn * turn)
            inverse = active[t, at] * (inverse * inverse)
            east[t, at] = (diag * re + turn * rn) * inverse
            north[t, at] = (diag * rn - turn * re) * inverse

    blocks = (high + MARGIN - low) // STEP
    gain = 1.0 + RELAX_RATE

    def subcycle(number, carried):
        growth, scale = carried

        stress_rows(low, growth)

        def both(block, _):
            start = pl.multiple_of(low + block * STEP, 8)
            stress_rows(start, growth)
            velocity_rows(start - STEP, scale)
            return 0

        lax.fori_loop(1, blocks, both, 0)
        velocity_rows(low + (blocks - 1) * STEP, scale)
        return growth * gain, scale * (1.0 / gain)

    lax.fori_loop(
        0, SUBCYCLES, subcycle, (jnp.float32(gain), jnp.float32(0.25 / gain))
    )

    shrink = 0.5 * gain**-SUBCYCLES
    own = slice(mid, high)
    for t in range(main):
        c = slice(t * LANES, (t + 1) * LANES)
        vel_out[0, :, c] = fields[1, :, c] = east[t, own]
        vel_out[1, :, c] = fields[2, :, c] = north[t, own]
        stress_out[0, :, c] = (plus[t, own] + minus[t, own]) * shrink
        stress_out[1, :, c] = (plus[t, own] - minus[t, own]) * shrink
        stress_out[2, :, c] = twice[t, own] * shrink
    for block in range(rows // STEP):
        add, sub, _, _ = gradients(mid + block * STEP)
        add_next = ahead(add)
        at = slice(block * STEP, (block + 1) * STEP)
        for t in range(main):
            c = slice(t * LANES, (t + 1) * LANES)
            value = conc[at, c]
            fields[0, at, c] = jnp.clip(value - value * (0.5 * (add_next[t] - sub[t])), 0.0, 1.0)


def ensemble_kernel(count, fields, mean, spread, landing, send_sem, recv_sem):
    me = lax.axis_index("ens")
    share = mean.shape[1]
    barrier = pltpu.get_barrier_semaphore()
    peers = [lax.rem(me + step, count) for step in range(1, count)]
    for peer in peers:
        pl.semaphore_signal(barrier, inc=1, device_id={"ens": peer}, device_id_type=MESH)
    pl.semaphore_wait(barrier, count - 1)
    copies = []
    for step, peer in enumerate(peers):
        each = pltpu.make_async_remote_copy(
            src_ref=fields.at[:, pl.ds(pl.multiple_of(peer * share, 8), share)],
            dst_ref=landing.at[step],
            send_sem=send_sem.at[step],
            recv_sem=recv_sem.at[step],
            device_id={"ens": peer},
            device_id_type=MESH,
        )
        each.start()
        copies.append(each)
    for each in copies:
        each.wait_recv()
    own = fields[:, pl.ds(pl.multiple_of(me * share, 8), share)]
    values = [own] + [landing[step] for step in range(count - 1)]
    average = functools.reduce(jnp.add, values) / count
    mean[...] = average
    spread[...] = functools.reduce(jnp.add, [(v - average) * (v - average) for v in values]) / count
    for each in copies:
        each.wait_send()


def solution(mesh):
    gx_count, gy_count, ens_count = mesh.shape["gx"], mesh.shape["gy"], mesh.shape["ens"]
    f32 = jnp.float32

    def vmem(*shape):
        return pltpu.VMEM(shape, f32)

    def specs(count):
        return [pl.BlockSpec(memory_space=pltpu.VMEM)] * count

    def body(velocity, stress, thickness, concentration, node_mass, wind, current, mask, ice):
        rows, cols = mask.shape
        vel, stress = velocity[0], stress[0]
        conc, mass, wind, current = concentration[0], node_mass[0], wind[0], current[0]
        up_rows, dn_rows = FIELDS * MARGIN + 2 * EXTRA, FIELDS * MARGIN
        cu_rows, cd_rows = C_TILES * MARGIN + EXTRA, C_TILES * MARGIN
        tall = rows + 2 * MARGIN + EXTRA
        shape = lambda *dims: jax.ShapeDtypeStruct(dims, f32)
        derived, halo, rows_lo, rows_hi = pl.pallas_call(
            functools.partial(exchange_kernel, (gx_count, gy_count)),
            name="halo_exchange",
            out_shape=(
                shape(2, rows, cols),
                shape(FIELDS, tall, LANES),
                shape(dn_rows, cols),
                shape(up_rows, cols),
            ),
            in_specs=specs(9),
            out_specs=tuple(specs(4)),
            scratch_shapes=[
                vmem(2, X_TILES, rows, LANES),
                vmem(2, X_TILES, rows, LANES),
                vmem(up_rows, cols),
                vmem(dn_rows, cols),
                vmem(up_rows, cols),
                vmem(dn_rows, cols),
                vmem(cu_rows, LANES),
                vmem(cd_rows, LANES),
                vmem(cu_rows, LANES),
                vmem(cd_rows, LANES),
                pltpu.SemaphoreType.DMA((6,)),
                pltpu.SemaphoreType.DMA((6,)),
            ],
            compiler_params=pltpu.CompilerParams(collective_id=0, has_side_effects=True, vmem_limit_bytes=16 << 20),
        )(vel, stress, thickness[0], conc, mass, wind, current, mask, ice[0])
        tiles = cols // LANES + 1
        vel_out, stress_out, fields = pl.pallas_call(
            functools.partial(subcycle_kernel, gy_count),
            name="subcycles",
            out_shape=(shape(2, rows, cols), shape(3, rows, cols), shape(3, rows, cols)),
            in_specs=specs(10),
            out_specs=tuple(specs(3)),
            scratch_shapes=[vmem(tiles, TOP + tall, LANES)] * 13,
            compiler_params=pltpu.CompilerParams(vmem_limit_bytes=20 << 20),
        )(vel, stress, derived, conc, mass, wind, current, halo, rows_lo, rows_hi)
        share = rows // ens_count
        mean, spread = pl.pallas_call(
            functools.partial(ensemble_kernel, ens_count),
            name="ensemble",
            out_shape=(shape(3, share, cols), shape(3, share, cols)),
            in_specs=specs(1),
            out_specs=tuple(specs(2)),
            scratch_shapes=[
                vmem(ens_count - 1, 3, share, cols),
                pltpu.SemaphoreType.DMA((ens_count - 1,)),
                pltpu.SemaphoreType.DMA((ens_count - 1,)),
            ],
            compiler_params=pltpu.CompilerParams(collective_id=1, has_side_effects=True, vmem_limit_bytes=6 << 20),
        )(fields)
        return vel_out[None], stress_out[None], mean, spread

    grid = P("ens", "gy", "gx")
    pair = P("ens", None, "gy", "gx")
    split = P(None, ("gy", "ens"), "gx")
    return jax.shard_map(
        body,
        mesh=mesh,
        in_specs=(pair, pair, grid, grid, grid, pair, pair, P("gy", "gx"), grid),
        out_specs=(pair, pair, split, split),
        check_vma=False,
    )
```
